32 devices in a mesh: fsdp: 16 (over z, x, core), tp: 2 (over y).
Axes of the slice: x: 2, y: 2, z: 4, core: 2. Of those that a mesh axis runs over, the one named last changes fastest.
Arguments:
- saved_master: float32 [16384, 5120], P(('fsdp', 'tp')), may hold values from -6 to 6
- saved_first: float32 [16384, 5120], P(('fsdp', 'tp')), may hold values from -6 to 6
- saved_second: float32 [16384, 5120], P(('fsdp', 'tp')), may hold values from 0.05 to 20
- grad: bfloat16 [16384, 5120], P('fsdp', 'tp'), may hold values from -10000 to 10000
- row_target: int32 [16384], replicated, may hold values from 0 to 16383, as said below
- step: int32 [1], replicated, may hold values from 1 to 63
Outputs:
- new_master: float32 [16384, 5120], P('fsdp', 'tp')
- new_first: float32 [16384, 5120], P('fsdp', 'tp')
- new_second: float32 [16384, 5120], P('fsdp', 'tp')
- direction: float32 [16384, 5120], P('fsdp', 'tp')
The draws below stay inside these ranges and needn't reach their ends.
Inputs may be any that keep to these rules, and one draw needn't show every extreme that they name: `row_target`: a permutation of 0 to 16383; the saved rows j * 1024 to (j + 1) * 1024 - 1 of every block j send exactly 64 rows into every new block of 1024 rows.
All inputs are finite; a program needn't handle non-finite values.
Results may differ from the reference program's by a relative error of at most 0.0003.
Values sent between devices are 32-bit elements; how exact they have to be, the bound alone decides.
No kernel may reach another device: no remote copies, remote signals or barrier semaphores. Data moves between devices by JAX's collectives and lax.ppermute only.
A program may use at most 192 MiB of HBM per device.

```python
import math
import jax
import jax.numpy as jnp

H = 16384
D = 5120
N_FSDP = 16


def draw_row_target(key, part):
    block_rows = H // N_FSDP
    pair_rows = block_rows // N_FSDP
    source_keys = jax.random.split(jax.random.fold_in(key, 11), N_FSDP)
    target_keys = jax.random.split(jax.random.fold_in(key, 12), N_FSDP)
    sigma = jax.vmap(lambda one: jax.random.permutation(one, block_rows))(source_keys).astype(jnp.int32)
    tau_table = jax.vmap(lambda one: jax.random.permutation(one, block_rows))(target_keys).astype(jnp.int32)
    target_block = sigma // pair_rows
    slot_index = sigma % pair_rows
    incoming = jnp.arange(N_FSDP, dtype=jnp.int32)[:, None] * pair_rows + slot_index
    local_row = tau_table.reshape(-1)[target_block * block_rows + incoming]
    return (target_block * block_rows + local_row).reshape(-1).astype(jnp.int32)


def draw_grad(key, part):
    row_key = jax.random.fold_in(key, 21)
    col_key = jax.random.fold_in(key, 22)
    base_key = jax.random.fold_in(key, 23)
    rising = 1.0 + 2.0 * jnp.arange(H, dtype=jnp.float32) / (H - 1)
    row_scale = jnp.exp(jax.random.uniform(row_key, (H, 1)) * math.log(10.0)) * rising[:, None]
    col_scale = jnp.exp(jax.random.uniform(col_key, (1, D)) * math.log(10.0))
    values = jax.random.normal(base_key, (H, D))
    return (values * row_scale * col_scale).astype(jnp.bfloat16)


def level_of(key, extent, cuts, low, largest):
    factor_of, own = 1.0, jax.random.fold_in(key, 6)
    for position, shards_of in cuts:
        heights = jnp.exp(jax.random.uniform(jax.random.fold_in(own, position), (shards_of,), jnp.float32, low / len(cuts), largest / len(cuts)))
        factor_of = factor_of * jnp.repeat(heights, extent[position] // shards_of).reshape([-1 if axis == position else 1 for axis in range(len(extent))])
    return factor_of


def scatter_about(stream_key, dims, deviation, reach, cuts=(), kind=jnp.bfloat16):
    array = jax.random.normal(stream_key, dims, jnp.float32) * deviation
    if len(cuts) > 0:
        array = level_of(stream_key, dims, cuts, -0.22, 0.18) * array
    return jnp.clip(array, min=-reach, max=reach).astype(kind)


def setup_inputs(seed: int = 0) -> dict:
    key_list = jax.random.split(jax.random.key(seed), 7)
    saved_master = scatter_about(key_list[0], (H, D), 1.0, 6.0, ((0, 32),), jnp.float32)
    saved_first = scatter_about(key_list[1], (H, D), 1.0, 6.0, ((0, 32),), jnp.float32)
    saved_second = jnp.clip(jnp.exp(math.log(20.0) - 5.9914645 * jax.random.uniform(key_list[2], (H, D), jnp.float32) ** level_of(key_list[2], (H, D), ((0, 32),), -0.2, 0.2)), 0.05, 20.0)
    grad = draw_grad(jax.random.fold_in(key_list[6], 71), 0)
    row_target = draw_row_target(jax.random.fold_in(key_list[6], 71), 0)
    step = jax.random.randint(key_list[5], (1,), 1, 64).astype(jnp.int32)
    return dict(saved_master=saved_master, saved_first=saved_first, saved_second=saved_second, grad=grad, row_target=row_target, step=step)


beta_one = 0.9
beta_two = 0.95
epsilon = 1e-08
learn_rate = 0.001
weight_decay = 0.1

def adam_update(master, first, second, grad, scale, step):
    clipped = scale * grad.astype(jnp.float32)
    first_new = beta_one * first + (1.0 - beta_one) * clipped
    second_new = beta_two * second + (1.0 - beta_two) * clipped * clipped
    count = step[0].astype(jnp.float32)
    first_hat = first_new / (1.0 - jnp.power(jnp.float32(beta_one), count))
    second_hat = second_new / (1.0 - jnp.power(jnp.float32(beta_two), count))
    direction = first_hat / (jnp.sqrt(second_hat) + epsilon) + weight_decay * master
    return (master - learn_rate * direction, first_new, second_new, direction)

def reference(saved_master, saved_first, saved_second, grad, row_target, step):
    master = jnp.zeros_like(saved_master).at[row_target].set(saved_master)
    first = jnp.zeros_like(saved_first).at[row_target].set(saved_first)
    second = jnp.zeros_like(saved_second).at[row_target].set(saved_second)
    grad_wide = grad.astype(jnp.float32)
    total = jnp.sum(grad_wide * grad_wide)
    scale = jnp.minimum(1.0, math.sqrt(H * D) / jnp.sqrt(total))
    return adam_update(master, first, second, grad, scale, step)
```

```python
import math

import jax
import jax.numpy as jnp
from jax import lax
from jax.sharding import PartitionSpec as P


beta_one = 0.9
beta_two = 0.95
epsilon = 1e-08
learn_rate = 0.001
weight_decay = 0.1
lanes = 128
early_shares = (0.2, 0.3, 0.5)
late_shares = (0.75, 0.25)


def column_cuts(columns, shares):
    units = max(columns // lanes, 1)
    edges = {0, columns}
    total = 0.0
    for share in shares[:-1]:
        total += share
        edges.add(min(max(round(total * units), 1), units - 1) * (columns // units))
    edges = sorted(edges)
    return list(zip(edges[:-1], edges[1:]))


def after(value, *others):
    return lax.optimization_barrier((value,) + others)[0]


def per_device(saved_master, saved_first, saved_second, grad, row_target, step):
    tp_count = lax.axis_size("tp")
    block_index = lax.axis_index("fsdp")
    tp_index = lax.axis_index("tp")
    block_rows, columns = grad.shape
    piece_rows = saved_master.shape[0]
    all_rows = row_target.shape[0]

    mine = lax.dynamic_slice_in_dim(row_target, block_index * block_rows, block_rows)
    send_order = jnp.argsort(mine, stable=True)
    piece = (tp_index - send_order // piece_rows) % tp_count
    send_order = piece * piece_rows + send_order % piece_rows

    def tp_start(saved, low, high, wait_for=None):
        parts = []
        for shift in range(1, tp_count):
            target = (tp_index + shift) % tp_count
            out = lax.dynamic_slice(saved, (0, target * columns + low), (piece_rows, high - low))
            if wait_for is not None:
                out = after(out, wait_for)
            ring = [(i, (i + shift) % tp_count) for i in range(tp_count)]
            parts.append(lax.ppermute(out, "tp", ring))
        return parts

    def rows_to_send(saved, low, high, parts):
        own = lax.dynamic_slice(saved, (0, tp_index * columns + low), (piece_rows, high - low))
        return jnp.concatenate([own] + parts, axis=0)[send_order]

    def exchange(rows):
        return lax.all_to_all(rows, "fsdp", split_axis=0, concat_axis=0, tiled=True)

    jobs = [("second", low, high) for low, high in column_cuts(columns, early_shares)]
    jobs += [("first", 0, columns)]
    jobs += [("master", low, high) for low, high in column_cuts(columns, late_shares)]
    saved = {"master": saved_master, "first": saved_first, "second": saved_second}

    lead = tp_start(saved[jobs[0][0]], *jobs[0][1:])
    grad_wide = grad.astype(jnp.float32)
    local_square = jnp.sum(grad_wide * grad_wide)
    total = lax.psum(local_square, ("fsdp", "tp"))
    scale = jnp.minimum(1.0, math.sqrt(all_rows * saved_master.shape[1]) / jnp.sqrt(total))

    parts = [lead] + [
        tp_start(saved[name], low, high, total)
        for job, (name, low, high) in enumerate(jobs)
        if job > 0
    ]
    arrived = {}
    previous = total
    for job, (name, low, high) in enumerate(jobs):
        rows = rows_to_send(saved[name], low, high, parts[job])
        rows = after(rows, previous)
        previous = exchange(rows)
        arrived.setdefault(name, []).append((low, high, previous))

    positions = jnp.arange(all_rows, dtype=jnp.int32)
    in_block = row_target // block_rows == block_index
    sort_keys = jnp.where(
        in_block, positions // block_rows * all_rows + row_target, all_rows * all_rows
    )
    picked = jnp.argsort(sort_keys, stable=True)[:block_rows]
    arrived_rows = row_target[picked] - block_index * block_rows
    place_order = jnp.argsort(arrived_rows, stable=True)

    def placed(name):
        return jnp.concatenate([rows[place_order] for _, _, rows in arrived[name]], axis=1)

    count = step[0].astype(jnp.float32)
    clipped = scale * grad.astype(jnp.float32)
    first_new = beta_one * placed("first") + (1.0 - beta_one) * clipped
    second_new = beta_two * placed("second") + (1.0 - beta_two) * clipped * clipped
    first_hat = first_new / (1.0 - jnp.power(jnp.float32(beta_one), count))
    second_hat = second_new / (1.0 - jnp.power(jnp.float32(beta_two), count))
    update = first_hat / (jnp.sqrt(second_hat) + epsilon)
    direction = None
    for low, high, rows in arrived["master"]:
        master = rows[place_order]
        part = update[:, low:high] + weight_decay * master
        moved = master - learn_rate * part
        if direction is None:
            rest = ((0, 0), (low, columns - high))
            direction, new_master = lax.optimization_barrier(
                (jnp.pad(part, rest), jnp.pad(moved, rest))
            )
        else:
            direction = lax.dynamic_update_slice(direction, part, (0, low))
            new_master = lax.dynamic_update_slice(new_master, moved, (0, low))
    return new_master, first_new, second_new, direction


def solution(mesh):
    in_specs = (
        P(("fsdp", "tp"), None),
        P(("fsdp", "tp"), None),
        P(("fsdp", "tp"), None),
        P("fsdp", "tp"),
        P(),
        P(),
    )
    out_specs = (P("fsdp", "tp"), P("fsdp", "tp"), P("fsdp", "tp"), P("fsdp", "tp"))
    return jax.shard_map(
        per_device, mesh=mesh, in_specs=in_specs, out_specs=out_specs, check_vma=False
    )
```

```python
import math

import jax
import jax.numpy as jnp
from jax import lax
from jax.sharding import PartitionSpec as P


beta_one = 0.9
beta_two = 0.95
epsilon = 1e-08
learn_rate = 0.001
weight_decay = 0.1
lanes = 128
early_shares = (0.2, 0.3, 0.5)
late_shares = (0.8, 0.2)


def column_cuts(columns, shares):
    units = max(columns // lanes, 1)
    edges = {0, columns}
    total = 0.0
    for share in shares[:-1]:
        total += share
        edges.add(min(max(round(total * units), 1), units - 1) * (columns // units))
    edges = sorted(edges)
    return list(zip(edges[:-1], edges[1:]))


def after(value, *others):
    return lax.optimization_barrier((value,) + others)[0]


def per_device(saved_master, saved_first, saved_second, grad, row_target, step):
    tp_count = lax.axis_size("tp")
    block_index = lax.axis_index("fsdp")
    tp_index = lax.axis_index("tp")
    fsdp_count = lax.axis_size("fsdp")
    block_rows, columns = grad.shape
    piece_rows = saved_master.shape[0]
    all_rows = row_target.shape[0]

    mine = lax.dynamic_slice_in_dim(row_target, block_index * block_rows, block_rows)
    send_order = jnp.argsort(mine, stable=True)
    piece = (tp_index - send_order // piece_rows) % tp_count
    send_order = piece * piece_rows + send_order % piece_rows

    def tp_start(saved, low, high):
        parts = []
        for shift in range(1, tp_count):
            target = (tp_index + shift) % tp_count
            out = lax.dynamic_slice(saved, (0, target * columns + low), (piece_rows, high - low))
            ring = [(i, (i + shift) % tp_count) for i in range(tp_count)]
            parts.append(lax.ppermute(out, "tp", ring))
        return parts

    def rows_to_send(saved, low, high, parts):
        own = lax.dynamic_slice(saved, (0, tp_index * columns + low), (piece_rows, high - low))
        return jnp.concatenate([own] + parts, axis=0)[send_order]

    def exchange(rows):
        return lax.all_to_all(rows, "fsdp", split_axis=0, concat_axis=0, tiled=True)

    jobs = [("second", low, high) for low, high in column_cuts(columns, early_shares)]
    jobs += [("first", 0, columns)]
    jobs += [("master", low, high) for low, high in column_cuts(columns, late_shares)]
    saved = {"master": saved_master, "first": saved_first, "second": saved_second}

    parts = [tp_start(saved[name], low, high) for name, low, high in jobs]
    grad_wide = grad.astype(jnp.float32)
    local_square = jnp.sum(grad_wide * grad_wide)
    copies = jnp.full((fsdp_count, 1), local_square, jnp.float32)
    copies = lax.all_to_all(copies, "fsdp", split_axis=0, concat_axis=0, tiled=True)
    column_square = jnp.sum(copies)
    total = column_square
    for shift in range(1, tp_count):
        ring = [(i, (i + shift) % tp_count) for i in range(tp_count)]
        total = total + lax.ppermute(column_square, "tp", ring)
    scale = jnp.minimum(1.0, math.sqrt(all_rows * saved_master.shape[1]) / jnp.sqrt(total))

    arrived = {"master": [], "first": [], "second": []}

    def run(job, *previous):
        name, low, high = jobs[job]
        rows = after(rows_to_send(saved[name], low, high, parts[job]), *previous)
        arrived[name].append((low, high, exchange(rows)))
        return arrived[name][-1][2]

    previous = column_square
    for job in range(len(jobs) - 1):
        previous = run(job, previous)

    positions = jnp.arange(all_rows, dtype=jnp.int32)
    in_block = row_target // block_rows == block_index
    sort_keys = jnp.where(
        in_block, positions // block_rows * all_rows + row_target, all_rows * all_rows
    )
    picked = jnp.argsort(sort_keys, stable=True)[:block_rows]
    arrived_rows = row_target[picked] - block_index * block_rows
    place_order = jnp.argsort(arrived_rows, stable=True)

    def placed(name):
        return jnp.concatenate([rows[place_order] for _, _, rows in arrived[name]], axis=1)

    count = step[0].astype(jnp.float32)
    clipped = scale * grad.astype(jnp.float32)
    first_new = beta_one * placed("first") + (1.0 - beta_one) * clipped
    second_new = beta_two * placed("second") + (1.0 - beta_two) * clipped * clipped
    first_hat = first_new / (1.0 - jnp.power(jnp.float32(beta_one), count))
    second_hat = second_new / (1.0 - jnp.power(jnp.float32(beta_two), count))
    update = first_hat / (jnp.sqrt(second_hat) + epsilon)
    run(len(jobs) - 1, previous, update)
    direction = None
    for low, high, rows in arrived["master"]:
        master = rows[place_order]
        part = update[:, low:high] + weight_decay * master
        moved = master - learn_rate * part
        if direction is None:
            rest = ((0, 0), (low, columns - high))
            direction, new_master = lax.optimization_barrier(
                (jnp.pad(part, rest), jnp.pad(moved, rest))
            )
        else:
            direction = lax.dynamic_update_slice(direction, part, (0, low))
            new_master = lax.dynamic_update_slice(new_master, moved, (0, low))
    return new_master, first_new, second_new, direction


def solution(mesh):
    in_specs = (
        P(("fsdp", "tp"), None),
        P(("fsdp", "tp"), None),
        P(("fsdp", "tp"), None),
        P("fsdp", "tp"),
        P(),
        P(),
    )
    out_specs = (P("fsdp", "tp"), P("fsdp", "tp"), P("fsdp", "tp"), P("fsdp", "tp"))
    return jax.shard_map(
        per_device, mesh=mesh, in_specs=in_specs, out_specs=out_specs, check_vma=False
    )
```
